256 devices in a mesh: seq: 128 (over z, y_hi, x, core), head: 2 (over y_lo).
Axes of the slice: x: 4, y: 4 (y_hi: 2, y_lo: 2; y = y_hi * 2 + y_lo), z: 8, core: 2. Of those that a mesh axis runs over, the one named last changes fastest.
Arguments:
- queries: bfloat16 [49152, 32, 128], P(('seq', 'head')), may hold values from -6 to 6
- keys: bfloat16 [49152, 8, 128], P('seq', 'head'), may hold values from -6 to 6
- values: bfloat16 [49152, 8, 128], P('seq', 'head'), may hold values from -1.5 to 1.5
- outputs: bfloat16 [49152, 32, 128], P(('seq', 'head')), may hold values from -1.5 to 1.5
- output_gradient: bfloat16 [49152, 32, 128], P(('seq', 'head')), may hold values from -24 to 24
- lse: float32 [49152, 32], P(('seq', 'head')), may hold values from 5.5 to 7.5
Outputs:
- query_grad: bfloat16 [49152, 32, 128], P(('seq', 'head'))
- key_gradient: bfloat16 [49152, 8, 128], P('seq', 'head')
- value_gradient: bfloat16 [49152, 8, 128], P('seq', 'head')
The draws below stay inside these ranges and needn't reach their ends.
All inputs are finite; a program needn't handle non-finite values.
Results may differ from the reference program's by a relative error of at most 0.0068.
Values may be sent and summed in bfloat16 or wider, within the bound.
A program may use at most 64 MiB of HBM per device.

```python
import jax
import jax.numpy as jnp
from jax import lax

QUERY_HEADS = 32
KEY_VALUE_HEADS = 8
HEAD_SIZE = 128
TOK_DEV = 384
WINDOW = 768
SEQUENCE_TOKENS = 49152
N_SEQ = 128


def steps_of(stream_key, dims, shards, least, largest):
    factor_of = 1.0
    for dim, shards_of in shards:
        draws = jax.random.uniform(jax.random.fold_in(jax.random.fold_in(stream_key, 6), dim), (shards_of,), jnp.float32, least / len(shards), largest / len(shards))
        factor_of = factor_of * jnp.repeat(jnp.exp(draws), dims[dim] // shards_of).reshape((-1,) + (1,) * (len(dims) - 1 - dim))
    return factor_of


def scatter_about(rng, shape, deviation, bound, pieces=(), held_as=jnp.bfloat16):
    array = jax.random.normal(rng, shape, jnp.float32) * deviation
    if len(pieces) > 0:
        array = steps_of(rng, shape, pieces, -0.22, 0.18) * array
    return jnp.clip(array, min=-bound, max=bound).astype(held_as)


def setup_inputs(seed: int = 0) -> dict:
    splits = jax.random.split(jax.random.key(seed), 7)
    return {
        "queries": scatter_about(splits[0], (SEQUENCE_TOKENS, QUERY_HEADS, HEAD_SIZE), 1.0, 6.0, ((0, 256),)),
        "keys": scatter_about(splits[1], (SEQUENCE_TOKENS, KEY_VALUE_HEADS, HEAD_SIZE), 1.0, 6.0, ((0, 128), (1, 2))),
        "values": scatter_about(splits[2], (SEQUENCE_TOKENS, KEY_VALUE_HEADS, HEAD_SIZE), 0.25, 1.5, ((0, 128), (1, 2))),
        "outputs": scatter_about(splits[3], (SEQUENCE_TOKENS, QUERY_HEADS, HEAD_SIZE), 0.25, 1.5, ((0, 256),)),
        "output_gradient": scatter_about(splits[4], (SEQUENCE_TOKENS, QUERY_HEADS, HEAD_SIZE), 4.0, 24.0, ((0, 256),)),
        "lse": jnp.clip(5.5 + 2.0 * jax.random.uniform(splits[5], (SEQUENCE_TOKENS, QUERY_HEADS), jnp.float32) ** steps_of(splits[5], (SEQUENCE_TOKENS, QUERY_HEADS), ((0, 256),), -0.2, 0.2), 5.5, 7.5),
    }


def block_grads(query_blk, grad_blk, output_blk, lse_blk, key_cat, value_cat, block_id):
    token_length = TOK_DEV
    score_scale = HEAD_SIZE ** -0.5
    row_ids = jnp.arange(token_length, dtype=jnp.int32)[:, None]
    col_ids = jnp.arange(3 * token_length, dtype=jnp.int32)[None, :]
    key_pos = block_id * token_length - 2 * token_length + col_ids
    allowed = (key_pos >= 0) & (col_ids > row_ids) & (col_ids <= row_ids + WINDOW)
    query_f = query_blk.astype(jnp.float32)
    grad_f = grad_blk.astype(jnp.float32)
    key_f = key_cat.astype(jnp.float32)
    value_f = value_cat.astype(jnp.float32)
    row_delta = jnp.sum(grad_f * output_blk.astype(jnp.float32), axis=-1)
    row_delta = jnp.transpose(row_delta, (1, 2, 0))[..., None]
    lse_part = jnp.transpose(lse_blk, (1, 2, 0))[..., None]
    scores = jnp.einsum('tkgd,ckd->kgtc', query_f, key_f) * score_scale
    attn_prob = jnp.where(allowed, jnp.exp(scores - lse_part), 0.0)
    prob_bf = lax.optimization_barrier(attn_prob.astype(jnp.bfloat16))
    value_part = jnp.einsum('kgtc,tkgd->ckd', prob_bf.astype(jnp.float32), grad_f)
    prob_grad = jnp.einsum('tkgd,ckd->kgtc', grad_f, value_f)
    score_bf = lax.optimization_barrier((attn_prob * (prob_grad - row_delta) * score_scale).astype(jnp.bfloat16))
    score_f = score_bf.astype(jnp.float32)
    query_grad = jnp.einsum('kgtc,ckd->tkgd', score_f, key_f).astype(jnp.bfloat16)
    key_part = jnp.einsum('kgtc,tkgd->ckd', score_f, query_f)
    return query_grad.reshape(token_length, QUERY_HEADS, HEAD_SIZE), key_part, value_part


def reference(queries, keys, values, outputs, output_gradient, lse):
    token_length = TOK_DEV
    number_of_blocks = N_SEQ
    query_groups = QUERY_HEADS // KEY_VALUE_HEADS
    query_stack = queries.reshape(number_of_blocks, token_length, KEY_VALUE_HEADS, query_groups, HEAD_SIZE)
    gradient_stack = output_gradient.reshape(number_of_blocks, token_length, KEY_VALUE_HEADS, query_groups, HEAD_SIZE)
    output_stack = outputs.reshape(number_of_blocks, token_length, KEY_VALUE_HEADS, query_groups, HEAD_SIZE)
    logsumexp_stack = lse.reshape(number_of_blocks, token_length, KEY_VALUE_HEADS, query_groups)
    key_padded = jnp.concatenate([jnp.zeros((2 * token_length, KEY_VALUE_HEADS, HEAD_SIZE), keys.dtype), keys], 0)
    value_padded = jnp.concatenate([jnp.zeros((2 * token_length, KEY_VALUE_HEADS, HEAD_SIZE), values.dtype), values], 0)

    def advance(carry, inputs):
        pend_key, pend_value = carry
        block_id, query_blk, grad_blk, output_blk, lse_blk = inputs
        start = (block_id * token_length).astype(jnp.int32)
        key_cat = lax.dynamic_slice_in_dim(key_padded, start, 3 * token_length, 0)
        value_cat = lax.dynamic_slice_in_dim(value_padded, start, 3 * token_length, 0)
        query_grad, key_part, value_part = block_grads(query_blk, grad_blk, output_blk, lse_blk, key_cat, value_cat, block_id)
        done_key = pend_key[0] + key_part[:token_length]
        done_value = pend_value[0] + value_part[:token_length]
        next_key = jnp.stack([pend_key[1] + key_part[token_length:2 * token_length], key_part[2 * token_length:]])
        next_value = jnp.stack([pend_value[1] + value_part[token_length:2 * token_length], value_part[2 * token_length:]])
        return (next_key, next_value), (query_grad, done_key, done_value)

    initial_carry = (jnp.zeros((2, token_length, KEY_VALUE_HEADS, HEAD_SIZE), jnp.float32), jnp.zeros((2, token_length, KEY_VALUE_HEADS, HEAD_SIZE), jnp.float32))
    block_ids = jnp.arange(number_of_blocks, dtype=jnp.int32)
    closing_carry, outputs_stacked = lax.scan(advance, initial_carry, (block_ids, query_stack, gradient_stack, output_stack, logsumexp_stack))
    query_grad = outputs_stacked[0].reshape(number_of_blocks * token_length, QUERY_HEADS, HEAD_SIZE)
    key_gradient = jnp.concatenate([outputs_stacked[1][2:].reshape(-1, KEY_VALUE_HEADS, HEAD_SIZE), closing_carry[0].reshape(-1, KEY_VALUE_HEADS, HEAD_SIZE)], 0)
    value_gradient = jnp.concatenate([outputs_stacked[2][2:].reshape(-1, KEY_VALUE_HEADS, HEAD_SIZE), closing_carry[1].reshape(-1, KEY_VALUE_HEADS, HEAD_SIZE)], 0)
    return query_grad, key_gradient.astype(jnp.bfloat16), value_gradient.astype(jnp.bfloat16)
```

```python
import jax
import jax.numpy as jnp
from jax import lax
from jax.experimental import pallas as pl
from jax.experimental.pallas import tpu as pltpu
from jax.sharding import PartitionSpec as P

MESH = pl.DeviceIdType.MESH
BLK = 384
HALF = 192
WIN = 960
OWN_HEADS = 4
HEADS = 8
GROUP = 768
CHUNK = 256
SCALE = 128**-0.5
LOG2E = 1.4426950408889634

NT = (((1,), (1,)), ((), ()))
NN = (((1,), (0,)), ((), ()))
TN = (((0,), (0,)), ((), ()))


def dot(a, b, dims):
    return lax.dot_general(a, b, dims, preferred_element_type=jnp.float32)


def kernel(n_seq, kv_in, q_ref, do_ref, lse_ref, dl_ref, dq_ref, dk_ref, dv_ref,
           kvbuf, gacc, r3buf, r2buf, r1buf, dbuf, xbuf, ybuf,
           f1_s, f1_r, f2_s, f2_r, f3_s, f3_r, r1_s, r1_r, r2_s, r2_r, r3_s, r3_r):
    seq = lax.axis_index("seq")
    y = lax.axis_index("head")
    core = lax.rem(seq, 2)
    col = lax.rem(lax.div(seq, 2), 4)
    first_col = (col == 0).astype(jnp.int32)
    last_col = (col == 3).astype(jnp.int32)
    off = y * HALF
    nxt = (lax.rem(seq + 2, n_seq), jnp.where(last_col == 1, 1 - y, y))
    prv = (lax.rem(seq + n_seq - 2, n_seq), jnp.where(first_col == 1, 1 - y, y))
    pair = (seq + 1 - 2 * core, y)
    mate = (seq, 1 - y)

    def own(m):
        return 4 * y + m

    def other(m):
        return 4 * (1 - y) + m

    def stage_head(i):
        early = jnp.where(jnp.where(i < 2, 0, 1) == first_col, own(lax.rem(i, 2)), other(lax.rem(i, 2)))
        late = jnp.where(lax.rem(i, 2) == 1, own(lax.div(i, 2)), other(lax.div(i, 2)))
        return jnp.where(i < 4, early, late)

    def back_head(k):
        early = jnp.where(k < 2, own(lax.rem(k, 2)), other(lax.rem(k, 2)))
        late = jnp.where(lax.rem(k + last_col, 2) == 1, own(lax.div(k, 2)), other(lax.div(k, 2)))
        return jnp.where(k < 4, early, late)

    def rc(src, dst, s, r, dev):
        return pltpu.make_async_remote_copy(src_ref=src, dst_ref=dst, send_sem=s, recv_sem=r,
                                            device_id=dev, device_id_type=MESH)

    def slot(g, n):
        return kvbuf.at[g, :, pl.ds(n * BLK, BLK), :]

    def f1(m):
        g = own(m)
        return rc(kv_in.at[m], slot(g, 2), f1_s.at[m], f1_r.at[m], mate)

    def f2(src, g):
        return rc(src, slot(g, 0), f2_s.at[g], f2_r.at[g], nxt)

    def f3(src, g):
        return rc(src, slot(g, 1), f3_s.at[g], f3_r.at[g], pair)

    def r3(g):
        return rc(r3buf.at[g], dbuf.at[g], r3_s.at[g], r3_r.at[g], pair)

    def r2(g):
        return rc(r2buf.at[g], xbuf.at[g], r2_s.at[g], r2_r.at[g], prv)

    def r1(m):
        return rc(r1buf.at[m], ybuf.at[m], r1_s.at[m], r1_r.at[m], mate)

    barrier = pltpu.get_barrier_semaphore()
    for dev in (nxt, prv, pair, mate):
        pl.semaphore_signal(barrier, inc=1, device_id=dev, device_id_type=MESH)
    pl.semaphore_wait(barrier, 4)

    for m in range(OWN_HEADS):
        f1(m).start()
    f2(kv_in.at[0], own(0)).start()
    f2(kv_in.at[1], own(1)).start()

    @pl.when(core == 0)
    def _():
        for m in range(OWN_HEADS):
            f3(kv_in.at[m], own(m)).start()

    def keep(m, carry):
        kvbuf[own(m), :, pl.ds(2 * BLK, BLK), :] = kv_in[m]
        return carry

    lax.fori_loop(0, OWN_HEADS, keep, 0)

    tile0 = 2 * seq + y - 4

    def compute(g):
        k = kvbuf[g, 0, pl.ds(off, WIN), :]
        v = kvbuf[g, 1, pl.ds(off, WIN), :]
        dk = dv = None
        for c in range(GROUP // CHUNK):
            sl = slice(c * CHUNK, (c + 1) * CHUNK)
            q = q_ref[g, sl, :]
            do = do_ref[g, sl, :]
            lse = lse_ref[g, :, sl]
            st = dot(k, q, NT) * (SCALE * LOG2E)
            lane = lax.broadcasted_iota(jnp.int32, (HALF, CHUNK), 1) + c * CHUNK
            tok = lane - HALF * ((lane >= HALF).astype(jnp.int32) + (lane >= 2 * HALF).astype(jnp.int32)
                                 + (lane >= 3 * HALF).astype(jnp.int32))
            low = lax.broadcasted_iota(jnp.int32, (HALF, CHUNK), 0) > tok
            parts = []
            for n in range(5):
                shift = lse + jnp.where(tile0 + n < 0, 1e30, 0.0)
                part = jnp.exp2(st[n * HALF:(n + 1) * HALF] - shift)
                if n == 0:
                    part = jnp.where(low, part, 0.0)
                if n == 4:
                    part = jnp.where(low, 0.0, part)
                parts.append(part)
            p = jnp.concatenate(parts, 0)
            ds = (p * (dot(v, do, NT) - dl_ref[g, :, sl])).astype(jnp.bfloat16)
            dv_c = dot(p.astype(jnp.bfloat16), do, NN)
            dk_c = dot(ds, q, NN)
            dv = dv_c if dv is None else dv + dv_c
            dk = dk_c if dk is None else dk + dk_c
            dq_ref[g, sl, :] = (dot(ds, k, TN) * SCALE).astype(jnp.bfloat16)
        gacc[g, 0, pl.ds(off, WIN), :] = dk * SCALE
        gacc[g, 1, pl.ds(off, WIN), :] = dv
        gacc[g, :, pl.ds((1 - y) * WIN, HALF), :] = jnp.zeros((2, HALF, 128), jnp.float32)

    def stage(i, carry):
        @pl.when(i < OWN_HEADS)
        def _():
            g = other(i)
            f1(i).wait_recv()
            f2(slot(g, 2), g).start()

            @pl.when(core == 0)
            def _():
                f3(slot(g, 2), g).start()

            @pl.when(i >= 2)
            def _():
                f2(kv_in.at[i], own(i)).start()

        @pl.when((i >= 1) & (i < 9))
        def _():
            g = stage_head(i - 1)
            r3(g).wait_recv()

            @pl.when(core == 1)
            def _():
                r2buf[g] = (gacc[g, :, pl.ds(0, BLK), :] + dbuf[g].astype(jnp.float32)).astype(jnp.bfloat16)
                r2(g).start()

            @pl.when(core == 0)
            def _():
                gacc[g, :, pl.ds(2 * BLK, BLK), :] += dbuf[g].astype(jnp.float32)

        @pl.when(i >= 3)
        def _():
            g = back_head(i - 3)
            r2(g).wait_recv()
            total = gacc[g, :, pl.ds(2 * BLK, BLK), :] + xbuf[g].astype(jnp.float32)
            mine = lax.div(g, 4) == y

            @pl.when(mine)
            def _():
                gacc[g, :, pl.ds(2 * BLK, BLK), :] = total

            @pl.when(jnp.logical_not(mine))
            def _():
                m = lax.rem(g, 4)
                r1buf[m] = total.astype(jnp.bfloat16)
                r1(m).start()

        @pl.when(i < HEADS)
        def _():
            g = stage_head(i)
            f2(slot(g, 2), g).wait_recv()

            @pl.when(core == 1)
            def _():
                f3(slot(g, 0), g).start()

            f3(slot(g, 0), g).wait_recv()
            compute(g)
            r3buf[g] = gacc[g, :, pl.ds(BLK, BLK), :].astype(jnp.bfloat16)

            @pl.when(core == 0)
            def _():
                r2buf[g] = gacc[g, :, pl.ds(0, BLK), :].astype(jnp.bfloat16)
                r2(g).start()

            r3(g).start()

        return carry

    lax.fori_loop(0, HEADS + 3, stage, 0)

    def finish(m, carry):
        r1(m).wait_recv()
        g = own(m)
        dk_ref[m] = (gacc[g, 0, pl.ds(2 * BLK, BLK), :] + ybuf[m, 0].astype(jnp.float32)).astype(jnp.bfloat16)
        dv_ref[m] = (gacc[g, 1, pl.ds(2 * BLK, BLK), :] + ybuf[m, 1].astype(jnp.float32)).astype(jnp.bfloat16)
        f1(m).wait_send()
        r1(m).wait_send()
        return carry

    lax.fori_loop(0, OWN_HEADS, finish, 0)

    def drain(g, carry):
        f2(slot(g, 2), g).wait_send()
        f3(slot(g, 2), g).wait_send()
        r2(g).wait_send()
        r3(g).wait_send()
        return carry

    lax.fori_loop(0, HEADS, drain, 0)


def attention_grads(n_seq, kv, q, do, lse, delta):
    vm = pl.BlockSpec(memory_space=pltpu.VMEM)
    bf, f32 = jnp.bfloat16, jnp.float32
    dma = pltpu.SemaphoreType.DMA
    return pl.pallas_call(
        lambda *refs: kernel(n_seq, *refs),
        out_shape=(
            jax.ShapeDtypeStruct((HEADS, GROUP, 128), bf),
            jax.ShapeDtypeStruct((OWN_HEADS, BLK, 128), bf),
            jax.ShapeDtypeStruct((OWN_HEADS, BLK, 128), bf),
        ),
        in_specs=[vm] * 5,
        out_specs=(vm, vm, vm),
        scratch_shapes=[
            pltpu.VMEM((HEADS, 2, 3 * BLK, 128), bf),
            pltpu.VMEM((HEADS, 2, 3 * BLK, 128), f32),
            pltpu.VMEM((HEADS, 2, BLK, 128), bf),
            pltpu.VMEM((HEADS, 2, BLK, 128), bf),
            pltpu.VMEM((OWN_HEADS, 2, BLK, 128), bf),
            pltpu.VMEM((HEADS, 2, BLK, 128), bf),
            pltpu.VMEM((HEADS, 2, BLK, 128), bf),
            pltpu.VMEM((OWN_HEADS, 2, BLK, 128), bf),
            dma((4,)), dma((4,)), dma((8,)), dma((8,)), dma((8,)), dma((8,)),
            dma((4,)), dma((4,)), dma((8,)), dma((8,)), dma((8,)), dma((8,)),
        ],
        compiler_params=pltpu.CompilerParams(
            collective_id=0, has_side_effects=True, vmem_limit_bytes=52 * 2**20
        ),
        name="window_grads",
    )(kv, q, do, lse, delta)


def body(n_seq, queries, keys, values, outputs, output_gradient, lse):
    delta = jnp.sum(output_gradient.astype(jnp.float32) * outputs.astype(jnp.float32), axis=-1)
    rows = lambda a: a.transpose(1, 0).reshape(HEADS, 1, GROUP)
    major = lambda a: a.transpose(1, 0, 2)
    kv = jnp.stack([major(keys), major(values)], 1)
    dq, dk, dv = attention_grads(
        n_seq, kv, major(queries).reshape(HEADS, GROUP, 128), major(output_gradient).reshape(HEADS, GROUP, 128),
        rows(lse) * LOG2E, rows(delta),
    )
    return major(dq.reshape(4 * HEADS, HALF, 128)), major(dk), major(dv)


def solution(mesh):
    n_seq = mesh.shape["seq"]
    return jax.shard_map(
        lambda *args: body(n_seq, *args),
        mesh=mesh,
        in_specs=(
            P(("seq", "head"), None, None),
            P("seq", "head", None),
            P("seq", "head", None),
            P(("seq", "head"), None, None),
            P(("seq", "head"), None, None),
            P(("seq", "head"), None),
        ),
        out_specs=(P(("seq", "head"), None, None), P("seq", "head", None), P("seq", "head", None)),
        check_vma=False,
    )
```

```python
import jax
import jax.numpy as jnp
from jax import lax
from jax.experimental import pallas as pl
from jax.experimental.pallas import tpu as pltpu
from jax.sharding import PartitionSpec as P

MESH = pl.DeviceIdType.MESH
BLK = 384
HALF = 192
WIN = 960
OWN_HEADS = 4
HEADS = 8
GROUP = 768
CHUNK = 256
LAG = 3
SCALE = 128**-0.5
LOG2E = 1.4426950408889634

NT = (((1,), (1,)), ((), ()))
NN = (((1,), (0,)), ((), ()))
TN = (((0,), (0,)), ((), ()))


def dot(a, b, dims):
    return lax.dot_general(a, b, dims, preferred_element_type=jnp.float32)


def kernel(n_seq, k_hbm, v_hbm, q_hbm, do_hbm, o_hbm, lse_hbm, dq_out, dk_ref, dv_ref,
           raw, raw_k, raw_v, lse_in, in_s, kv_in, kv_out, q_ref, do_ref, o_ref, lse_ref, dq_ref, kvbuf, gacc, r3buf, r2buf, r1buf, dbuf, xbuf, ybuf,
           f1_s, f1_r, f2_s, f2_r, f3_s, f3_r, r1_s, r1_r, r2_s, r2_r, r3_s, r3_r):
    seq = lax.axis_index("seq")
    y = lax.axis_index("head")
    core = lax.rem(seq, 2)
    col = lax.rem(lax.div(seq, 2), 4)
    first_col = (col == 0).astype(jnp.int32)
    last_col = (col == 3).astype(jnp.int32)
    off = y * HALF
    starts = seq < 2
    ends = seq >= n_seq - 2
    nxt = (lax.rem(seq + 2, n_seq), jnp.where(last_col == 1, 1 - y, y))
    prv = (lax.rem(seq + n_seq - 2, n_seq), jnp.where(first_col == 1, 1 - y, y))
    pair = (seq + 1 - 2 * core, y)
    mate = (seq, 1 - y)

    def own(m):
        return 4 * y + m

    def other(m):
        return 4 * (1 - y) + m

    def stage_head(i):
        early = jnp.where(jnp.where(i < 2, 0, 1) == first_col, own(lax.rem(i, 2)), other(lax.rem(i, 2)))
        late = jnp.where(jnp.where(i < 6, 1, 0) == first_col, own(2 + lax.rem(i, 2)), other(2 + lax.rem(i, 2)))
        return jnp.where(i < 4, early, late)

    def back_head(k):
        early = jnp.where(k < 2, own(lax.rem(k, 2)), other(lax.rem(k, 2)))
        late = jnp.where(k < 6, other(2 + lax.rem(k, 2)), own(2 + lax.rem(k, 2)))
        return jnp.where(k < 4, early, late)

    def rc(src, dst, s, r, dev):
        return pltpu.make_async_remote_copy(src_ref=src, dst_ref=dst, send_sem=s, recv_sem=r,
                                            device_id=dev, device_id_type=MESH)

    def slot(g, n):
        return kvbuf.at[g, :, pl.ds(n * BLK, BLK), :]

    def f1(m):
        g = own(m)
        return rc(kv_in.at[m], slot(g, 2), f1_s.at[m], f1_r.at[m], mate)

    def f2(src, g):
        return rc(src, slot(g, 0), f2_s.at[g], f2_r.at[g], nxt)

    def f3(src, g):
        return rc(src, slot(g, 1), f3_s.at[g], f3_r.at[g], pair)

    def r3(g):
        return rc(r3buf.at[g], dbuf.at[g], r3_s.at[g], r3_r.at[g], pair)

    def r2(g):
        return rc(r2buf.at[g], xbuf.at[g], r2_s.at[g], r2_r.at[g], prv)

    def r1(m):
        return rc(r1buf.at[m], ybuf.at[m], r1_s.at[m], r1_r.at[m], mate)

    loads = [pltpu.make_async_copy(src, dst, in_s.at[n]) for n, (src, dst) in enumerate((
        (q_hbm, raw.at[0]), (do_hbm, raw.at[1]), (o_hbm, raw.at[2]), (k_hbm, raw_k), (v_hbm, raw_v), (lse_hbm, lse_in)))]
    for load in loads[3:5] + loads[:3] + loads[5:]:
        load.start()
    barrier = pltpu.get_barrier_semaphore()
    for dev, skip in ((nxt, ends), (prv, starts), (pair, None), (mate, None)):
        def greet(dev=dev):
            pl.semaphore_signal(barrier, inc=1, device_id=dev, device_id_type=MESH)

        if skip is None:
            greet()
        else:
            pl.when(jnp.logical_not(skip))(greet)
    for n, src in enumerate((raw_k, raw_v)):
        loads[3 + n].wait()
        kv_in[:, n] = jnp.transpose(src[...], (1, 0, 2))
    pl.semaphore_wait(barrier, jnp.where(starts | ends, 3, 4))

    for m in range(OWN_HEADS):
        f1(m).start()

    @pl.when(jnp.logical_not(ends))
    def _():
        f2(kv_in.at[0], own(0)).start()
        f2(kv_in.at[1], own(1)).start()

    @pl.when(core == 0)
    def _():
        for m in range(OWN_HEADS):
            f3(kv_in.at[m], own(m)).start()

    def keep(m, carry):
        kvbuf[own(m), :, pl.ds(2 * BLK, BLK), :] = kv_in[m]
        return carry

    lax.fori_loop(0, OWN_HEADS, keep, 0)

    @pl.when(starts)
    def _():
        def clear(g, carry):
            kvbuf[g, :, pl.ds(0, BLK), :] = jnp.zeros((2, BLK, 128), jnp.bfloat16)
            return carry

        lax.fori_loop(0, HEADS, clear, 0)

    for n, dst in enumerate((q_ref, do_ref, o_ref)):
        loads[n].wait()
        dst[...] = jnp.transpose(raw[n], (1, 0, 2)).reshape(HEADS, GROUP, 128)
    loads[5].wait()
    for h in range(4 * HEADS):
        lse_ref[h // 4, :, h % 4 * HALF:(h % 4 + 1) * HALF] = lse_in[h:h + 1, :] * LOG2E

    tile0 = 2 * seq + y - 4

    def compute(g):
        k = kvbuf[g, 0, pl.ds(off, WIN), :]
        v = kvbuf[g, 1, pl.ds(off, WIN), :]
        dk = dv = None
        for c in range(GROUP // CHUNK):
            sl = slice(c * CHUNK, (c + 1) * CHUNK)
            q = q_ref[g, sl, :]
            do = do_ref[g, sl, :]
            lse = lse_ref[g, :, sl]
            st = dot(k, q, NT) * (SCALE * LOG2E)
            lane = lax.broadcasted_iota(jnp.int32, (HALF, CHUNK), 1) + c * CHUNK
            tok = lane - HALF * ((lane >= HALF).astype(jnp.int32) + (lane >= 2 * HALF).astype(jnp.int32)
                                 + (lane >= 3 * HALF).astype(jnp.int32))
            low = lax.broadcasted_iota(jnp.int32, (HALF, CHUNK), 0) > tok
            parts = []
            for n in range(5):
                shift = lse + jnp.where(tile0 + n < 0, 1e30, 0.0)
                part = jnp.exp2(st[n * HALF:(n + 1) * HALF] - shift)
                if n == 0:
                    part = jnp.where(low, part, 0.0)
                if n == 4:
                    part = jnp.where(low, 0.0, part)
                parts.append(part)
            p = jnp.concatenate(parts, 0)
            prod = do.astype(jnp.float32) * o_ref[g, sl, :].astype(jnp.float32)
            high = prod.astype(jnp.bfloat16)
            rest = (prod - high.astype(jnp.float32)).astype(jnp.bfloat16)
            ones = jnp.ones((16, 128), jnp.bfloat16)
            delta = (dot(ones, high, NT) + dot(ones, rest, NT))[:1]
            ds = (p * (dot(v, do, NT) - delta)).astype(jnp.bfloat16)
            dv_c = dot(p.astype(jnp.bfloat16), do, NN)
            dk_c = dot(ds, q, NN)
            dv = dv_c if dv is None else dv + dv_c
            dk = dk_c if dk is None else dk + dk_c
            dq_ref[g, sl, :] = (dot(ds, k, TN) * SCALE).astype(jnp.bfloat16)
        gacc[g, 0, pl.ds(off, WIN), :] = dk * SCALE
        gacc[g, 1, pl.ds(off, WIN), :] = dv
        gacc[g, :, pl.ds((1 - y) * WIN, HALF), :] = jnp.zeros((2, HALF, 128), jnp.float32)

    def stage(i, carry):
        @pl.when(i < OWN_HEADS)
        def _():
            g = other(i)
            f1(i).wait_recv()

            @pl.when(jnp.logical_not(ends))
            def _():
                f2(slot(g, 2), g).start()

                @pl.when(i == 3)
                def _():
                    f2(kv_in.at[2], own(2)).start()
                    f2(kv_in.at[3], own(3)).start()

            @pl.when(core == 0)
            def _():
                f3(slot(g, 2), g).start()

        @pl.when(i < HEADS)
        def _():
            g = stage_head(i)

            @pl.when(jnp.logical_not(starts))
            def _():
                f2(slot(g, 2), g).wait_recv()

            @pl.when(core == 1)
            def _():
                f3(slot(g, 0), g).start()

        @pl.when((i >= 1) & (i < 9))
        def _():
            g = stage_head(i - 1)
            r3(g).wait_recv()

            @pl.when((core == 1) & jnp.logical_not(starts))
            def _():
                r2buf[g] = (gacc[g, :, pl.ds(0, BLK), :] + dbuf[g].astype(jnp.float32)).astype(jnp.bfloat16)
                r2(g).start()

            @pl.when(core == 0)
            def _():
                gacc[g, :, pl.ds(2 * BLK, BLK), :] += dbuf[g].astype(jnp.float32)

        @pl.when(i >= LAG)
        def _():
            g = back_head(i - LAG)

            @pl.when(jnp.logical_not(ends))
            def _():
                r2(g).wait_recv()
                gacc[g, :, pl.ds(2 * BLK, BLK), :] += xbuf[g].astype(jnp.float32)

            @pl.when(lax.div(g, 4) != y)
            def _():
                m = lax.rem(g, 4)
                r1buf[m] = gacc[g, :, pl.ds(2 * BLK, BLK), :].astype(jnp.bfloat16)
                r1(m).start()

        @pl.when(i < HEADS)
        def _():
            g = stage_head(i)
            f3(slot(g, 0), g).wait_recv()
            compute(g)
            r3buf[g] = gacc[g, :, pl.ds(BLK, BLK), :].astype(jnp.bfloat16)

            @pl.when((core == 0) & jnp.logical_not(starts))
            def _():
                r2buf[g] = gacc[g, :, pl.ds(0, BLK), :].astype(jnp.bfloat16)
                r2(g).start()

            r3(g).start()

        @pl.when(i == HEADS)
        def _():
            dq_out[...] = jnp.transpose(dq_ref[...].reshape(4 * HEADS, HALF, 128), (1, 0, 2))

        return carry

    lax.fori_loop(0, HEADS + LAG, stage, 0)

    def finish(m, carry):
        r1(m).wait_recv()
        g = own(m)
        kv_out[m] = (gacc[g, :, pl.ds(2 * BLK, BLK), :] + ybuf[m].astype(jnp.float32)).astype(jnp.bfloat16)
        f1(m).wait_send()
        r1(m).wait_send()
        return carry

    lax.fori_loop(0, OWN_HEADS, finish, 0)

    def drain(g, carry):
        @pl.when(jnp.logical_not(ends))
        def _():
            f2(slot(g, 2), g).wait_send()

        @pl.when(jnp.logical_not(starts))
        def _():
            r2(g).wait_send()

        f3(slot(g, 2), g).wait_send()
        r3(g).wait_send()
        return carry

    lax.fori_loop(0, HEADS, drain, 0)
    dk_ref[...] = jnp.transpose(kv_out[:, 0], (1, 0, 2))
    dv_ref[...] = jnp.transpose(kv_out[:, 1], (1, 0, 2))


def store(a_ref, b_ref, c_ref, a_out, b_out, c_out, sem):
    copies = [pltpu.make_async_copy(src, dst, sem.at[n])
              for n, (src, dst) in enumerate(((a_ref, a_out), (b_ref, b_out), (c_ref, c_out)))]
    for copy in copies:
        copy.start()
    for copy in copies:
        copy.wait()


def attention_grads(n_seq, k, v, q, do, o, lse):
    vm, hbm = pl.BlockSpec(memory_space=pltpu.VMEM), pl.BlockSpec(memory_space=pltpu.HBM)
    bf, f32 = jnp.bfloat16, jnp.float32
    dma = pltpu.SemaphoreType.DMA
    shapes = (
        jax.ShapeDtypeStruct((HALF, 4 * HEADS, 128), bf),
        jax.ShapeDtypeStruct((BLK, OWN_HEADS, 128), bf),
        jax.ShapeDtypeStruct((BLK, OWN_HEADS, 128), bf),
    )
    grads = pl.pallas_call(
        lambda *refs: kernel(n_seq, *refs),
        out_shape=shapes,
        in_specs=[hbm] * 6,
        out_specs=(vm, vm, vm),
        scratch_shapes=[
            pltpu.VMEM((3, HALF, 4 * HEADS, 128), bf),
            pltpu.VMEM((BLK, OWN_HEADS, 128), bf),
            pltpu.VMEM((BLK, OWN_HEADS, 128), bf),
            pltpu.VMEM((4 * HEADS, HALF), f32),
            dma((6,)),
            pltpu.VMEM((OWN_HEADS, 2, BLK, 128), bf),
            pltpu.VMEM((OWN_HEADS, 2, BLK, 128), bf),
            pltpu.VMEM((HEADS, GROUP, 128), bf),
            pltpu.VMEM((HEADS, GROUP, 128), bf),
            pltpu.VMEM((HEADS, GROUP, 128), bf),
            pltpu.VMEM((HEADS, 1, GROUP), f32),
            pltpu.VMEM((HEADS, GROUP, 128), bf),
            pltpu.VMEM((HEADS, 2, 3 * BLK, 128), bf),
            pltpu.VMEM((HEADS, 2, 3 * BLK, 128), f32),
            pltpu.VMEM((HEADS, 2, BLK, 128), bf),
            pltpu.VMEM((HEADS, 2, BLK, 128), bf),
            pltpu.VMEM((OWN_HEADS, 2, BLK, 128), bf),
            pltpu.VMEM((HEADS, 2, BLK, 128), bf),
            pltpu.VMEM((HEADS, 2, BLK, 128), bf),
            pltpu.VMEM((OWN_HEADS, 2, BLK, 128), bf),
            dma((4,)), dma((4,)), dma((8,)), dma((8,)), dma((8,)), dma((8,)),
            dma((4,)), dma((4,)), dma((8,)), dma((8,)), dma((8,)), dma((8,)),
        ],
        compiler_params=pltpu.CompilerParams(
            collective_id=0, has_side_effects=True, vmem_limit_bytes=50 * 2**20
        ),
        name="window_grads",
    )(*(pltpu.with_memory_space_constraint(a, pltpu.HBM) for a in (k, v, q, do, o, lse)))
    return pl.pallas_call(
        store,
        out_shape=shapes,
        in_specs=[vm] * 3,
        out_specs=(hbm, hbm, hbm),
        scratch_shapes=[dma((3,))],
        compiler_params=pltpu.CompilerParams(vmem_limit_bytes=8 * 2**20),
        name="store_grads",
    )(*grads)


def body(n_seq, queries, keys, values, outputs, output_gradient, lse):
    return attention_grads(n_seq, keys, values, queries, output_gradient, outputs, lse.transpose(1, 0))


def solution(mesh):
    n_seq = mesh.shape["seq"]
    return jax.shard_map(
        lambda *args: body(n_seq, *args),
        mesh=mesh,
        in_specs=(
            P(("seq", "head"), None, None),
            P("seq", "head", None),
            P("seq", "head", None),
            P(("seq", "head"), None, None),
            P(("seq", "head"), None, None),
            P(("seq", "head"), None),
        ),
        out_specs=(P(("seq", "head"), None, None), P("seq", "head", None), P("seq", "head", None)),
        check_vma=False,
    )
```

```python
import jax
import jax.numpy as jnp
from jax import lax
from jax.experimental import pallas as pl
from jax.experimental.pallas import tpu as pltpu
from jax.sharding import PartitionSpec as P

MESH = pl.DeviceIdType.MESH
BLK = 384
HALF = 192
WIN = 960
OWN_HEADS = 4
HEADS = 8
GROUP = 768
CHUNK = 256
LAG = 3
SCALE = 128**-0.5
LOG2E = 1.4426950408889634

NT = (((1,), (1,)), ((), ()))
NN = (((1,), (0,)), ((), ()))
TN = (((0,), (0,)), ((), ()))


def dot(a, b, dims):
    return lax.dot_general(a, b, dims, preferred_element_type=jnp.float32)


def kernel(n_seq, k_hbm, v_hbm, q_hbm, do_hbm, o_hbm, lse_hbm, dq_out, dk_ref, dv_ref,
           raw, raw_k, raw_v, lse_in, in_s, kv_in, kv_out, q_ref, do_ref, o_ref, lse_ref, dl_ref, dq_ref, kvbuf, gacc, r3buf, r2buf, r1buf, dbuf, xbuf, ybuf,
           f1_s, f1_r, f2_s, f2_r, f3_s, f3_r, r1_s, r1_r, r2_s, r2_r, r3_s, r3_r):
    seq = lax.axis_index("seq")
    y = lax.axis_index("head")
    core = lax.rem(seq, 2)
    col = lax.rem(lax.div(seq, 2), 4)
    first_col = (col == 0).astype(jnp.int32)
    last_col = (col == 3).astype(jnp.int32)
    off = y * HALF
    starts = seq < 2
    ends = seq >= n_seq - 2
    nxt = (lax.rem(seq + 2, n_seq), jnp.where(last_col == 1, 1 - y, y))
    prv = (lax.rem(seq + n_seq - 2, n_seq), jnp.where(first_col == 1, 1 - y, y))
    pair = (seq + 1 - 2 * core, y)
    mate = (seq, 1 - y)

    def own(m):
        return 4 * y + m

    def other(m):
        return 4 * (1 - y) + m

    def stage_head(i):
        early = jnp.where(jnp.where(i < 2, 0, 1) == first_col, own(lax.rem(i, 2)), other(lax.rem(i, 2)))
        late = jnp.where(jnp.where(i < 6, 1, 0) == first_col, own(2 + lax.rem(i, 2)), other(2 + lax.rem(i, 2)))
        return jnp.where(i < 4, early, late)

    def back_head(k):
        early = jnp.where(k < 2, own(lax.rem(k, 2)), other(lax.rem(k, 2)))
        late = jnp.where(k < 6, other(2 + lax.rem(k, 2)), own(2 + lax.rem(k, 2)))
        return jnp.where(k < 4, early, late)

    def rc(src, dst, s, r, dev):
        return pltpu.make_async_remote_copy(src_ref=src, dst_ref=dst, send_sem=s, recv_sem=r,
                                            device_id=dev, device_id_type=MESH)

    def slot(g, n):
        return kvbuf.at[g, :, pl.ds(n * BLK, BLK), :]

    def f1(m):
        g = own(m)
        return rc(kv_in.at[m], slot(g, 2), f1_s.at[m], f1_r.at[m], mate)

    def f2(src, g):
        return rc(src, slot(g, 0), f2_s.at[g], f2_r.at[g], nxt)

    def f3(src, g):
        return rc(src, slot(g, 1), f3_s.at[g], f3_r.at[g], pair)

    def r3(g):
        return rc(r3buf.at[g], dbuf.at[g], r3_s.at[g], r3_r.at[g], pair)

    def r2(g):
        return rc(r2buf.at[g], xbuf.at[g], r2_s.at[g], r2_r.at[g], prv)

    def r1(m):
        return rc(r1buf.at[m], ybuf.at[m], r1_s.at[m], r1_r.at[m], mate)

    loads = [pltpu.make_async_copy(src, dst, in_s.at[n]) for n, (src, dst) in enumerate((
        (q_hbm, raw.at[0]), (do_hbm, raw.at[1]), (o_hbm, raw.at[2]), (k_hbm, raw_k), (v_hbm, raw_v), (lse_hbm, lse_in)))]
    for load in loads[3:5] + loads[:3] + loads[5:]:
        load.start()
    barrier = pltpu.get_barrier_semaphore()
    for dev, skip in ((nxt, ends), (prv, starts), (pair, None), (mate, None)):
        def greet(dev=dev):
            pl.semaphore_signal(barrier, inc=1, device_id=dev, device_id_type=MESH)

        if skip is None:
            greet()
        else:
            pl.when(jnp.logical_not(skip))(greet)
    for n, src in enumerate((raw_k, raw_v)):
        loads[3 + n].wait()
        kv_in[:, n] = jnp.transpose(src[...], (1, 0, 2))
    pl.semaphore_wait(barrier, jnp.where(starts | ends, 3, 4))

    for m in range(OWN_HEADS):
        f1(m).start()

    @pl.when(jnp.logical_not(ends))
    def _():
        f2(kv_in.at[0], own(0)).start()
        f2(kv_in.at[1], own(1)).start()

    @pl.when(core == 0)
    def _():
        for m in range(OWN_HEADS):
            f3(kv_in.at[m], own(m)).start()

    def keep(m, carry):
        kvbuf[own(m), :, pl.ds(2 * BLK, BLK), :] = kv_in[m]
        return carry

    lax.fori_loop(0, OWN_HEADS, keep, 0)

    @pl.when(starts)
    def _():
        def clear(g, carry):
            kvbuf[g, :, pl.ds(0, BLK), :] = jnp.zeros((2, BLK, 128), jnp.bfloat16)
            return carry

        lax.fori_loop(0, HEADS, clear, 0)

    for n, dst in enumerate((q_ref, do_ref, o_ref)):
        loads[n].wait()
        dst[...] = jnp.transpose(raw[n], (1, 0, 2)).reshape(HEADS, GROUP, 128)
    loads[5].wait()
    for h in range(4 * HEADS):
        lse_ref[h // 4, :, h % 4 * HALF:(h % 4 + 1) * HALF] = lse_in[h:h + 1, :] * LOG2E

    def row_sums(g, carry):
        prod = do_ref[g].astype(jnp.float32) * o_ref[g].astype(jnp.float32)
        high = prod.astype(jnp.bfloat16)
        rest = (prod - high.astype(jnp.float32)).astype(jnp.bfloat16)
        ones = jnp.ones((16, 128), jnp.bfloat16)
        dl_ref[g] = (dot(ones, high, NT) + dot(ones, rest, NT))[:1]
        gacc[g, :, pl.ds((1 - y) * WIN, HALF), :] = jnp.zeros((2, HALF, 128), jnp.float32)
        return carry

    lax.fori_loop(0, HEADS, row_sums, 0)
    tile0 = 2 * seq + y - 4

    def compute(g):
        k = kvbuf[g, 0, pl.ds(off, WIN), :]
        v = kvbuf[g, 1, pl.ds(off, WIN), :]
        dk = dv = None
        for c in range(GROUP // CHUNK):
            sl = slice(c * CHUNK, (c + 1) * CHUNK)
            q = q_ref[g, sl, :]
            do = do_ref[g, sl, :]
            lse = lse_ref[g, :, sl]
            st = dot(k, q, NT) * (SCALE * LOG2E)
            lane = lax.broadcasted_iota(jnp.int32, (HALF, CHUNK), 1) + c * CHUNK
            tok = lane - HALF * ((lane >= HALF).astype(jnp.int32) + (lane >= 2 * HALF).astype(jnp.int32)
                                 + (lane >= 3 * HALF).astype(jnp.int32))
            low = lax.broadcasted_iota(jnp.int32, (HALF, CHUNK), 0) > tok
            parts = []
            for n in range(5):
                shift = lse + jnp.where(tile0 + n < 0, 1e30, 0.0)
                part = jnp.exp2(st[n * HALF:(n + 1) * HALF] - shift)
                if n == 0:
                    part = jnp.where(low, part, 0.0)
                if n == 4:
                    part = jnp.where(low, 0.0, part)
                parts.append(part)
            p = jnp.concatenate(parts, 0)
            ds = (p * (dot(v, do, NT) - dl_ref[g, :, sl])).astype(jnp.bfloat16)
            dv_c = dot(p.astype(jnp.bfloat16), do, NN)
            dk_c = dot(ds, q, NN)
            dv = dv_c if dv is None else dv + dv_c
            dk = dk_c if dk is None else dk + dk_c
            dq_ref[g, sl, :] = (dot(ds, k, TN) * SCALE).astype(jnp.bfloat16)
        gacc[g, 0, pl.ds(off, WIN), :] = dk * SCALE
        gacc[g, 1, pl.ds(off, WIN), :] = dv

    def add_returned(i):
        g = back_head(i - LAG)

        @pl.when(jnp.logical_not(ends))
        def _():
            r2(g).wait_recv()
            gacc[g, :, pl.ds(2 * BLK, BLK), :] += xbuf[g].astype(jnp.float32)

        @pl.when(lax.div(g, 4) != y)
        def _():
            m = lax.rem(g, 4)
            r1buf[m] = gacc[g, :, pl.ds(2 * BLK, BLK), :].astype(jnp.bfloat16)
            r1(m).start()

    def stage(i, carry):
        @pl.when(i < OWN_HEADS)
        def _():
            g = other(i)
            f1(i).wait_recv()

            @pl.when(jnp.logical_not(ends))
            def _():
                f2(slot(g, 2), g).start()

                @pl.when(i == 3)
                def _():
                    f2(kv_in.at[2], own(2)).start()
                    f2(kv_in.at[3], own(3)).start()

            @pl.when(core == 0)
            def _():
                f3(slot(g, 2), g).start()

        @pl.when(i < HEADS)
        def _():
            g = stage_head(i)

            @pl.when(jnp.logical_not(starts))
            def _():
                f2(slot(g, 2), g).wait_recv()

            @pl.when(core == 1)
            def _():
                f3(slot(g, 0), g).start()

        early = (core == 1) & (i >= 0)

        @pl.when((i >= LAG) & early)
        def _():
            add_returned(i)

        @pl.when((i >= 1) & (i < 9))
        def _():
            g = stage_head(i - 1)
            r3(g).wait_recv()

            @pl.when((core == 1) & jnp.logical_not(starts))
            def _():
                r2buf[g] = (gacc[g, :, pl.ds(0, BLK), :] + dbuf[g].astype(jnp.float32)).astype(jnp.bfloat16)
                r2(g).start()

            @pl.when(core == 0)
            def _():
                gacc[g, :, pl.ds(2 * BLK, BLK), :] += dbuf[g].astype(jnp.float32)

        @pl.when((i >= LAG) & jnp.logical_not(early))
        def _():
            add_returned(i)

        @pl.when(i < HEADS)
        def _():
            g = stage_head(i)
            f3(slot(g, 0), g).wait_recv()
            compute(g)
            r3buf[g] = gacc[g, :, pl.ds(BLK, BLK), :].astype(jnp.bfloat16)

            @pl.when((core == 0) & jnp.logical_not(starts))
            def _():
                r2buf[g] = gacc[g, :, pl.ds(0, BLK), :].astype(jnp.bfloat16)
                r2(g).start()

            r3(g).start()

        @pl.when(i == HEADS)
        def _():
            dq_out[...] = jnp.transpose(dq_ref[...].reshape(4 * HEADS, HALF, 128), (1, 0, 2))

        return carry

    lax.fori_loop(0, HEADS + LAG, stage, 0)

    def finish(m, carry):
        r1(m).wait_recv()
        g = own(m)
        kv_out[m] = (gacc[g, :, pl.ds(2 * BLK, BLK), :] + ybuf[m].astype(jnp.float32)).astype(jnp.bfloat16)
        f1(m).wait_send()
        r1(m).wait_send()
        return carry

    lax.fori_loop(0, OWN_HEADS, finish, 0)

    def drain(g, carry):
        @pl.when(jnp.logical_not(ends))
        def _():
            f2(slot(g, 2), g).wait_send()

        @pl.when(jnp.logical_not(starts))
        def _():
            r2(g).wait_send()

        f3(slot(g, 2), g).wait_send()
        r3(g).wait_send()
        return carry

    lax.fori_loop(0, HEADS, drain, 0)
    dk_ref[...] = jnp.transpose(kv_out[:, 0], (1, 0, 2))
    dv_ref[...] = jnp.transpose(kv_out[:, 1], (1, 0, 2))


def store(a_ref, b_ref, c_ref, a_out, b_out, c_out, sem):
    copies = [pltpu.make_async_copy(src, dst, sem.at[n])
              for n, (src, dst) in enumerate(((a_ref, a_out), (b_ref, b_out), (c_ref, c_out)))]
    for copy in copies:
        copy.start()
    for copy in copies:
        copy.wait()


def attention_grads(n_seq, k, v, q, do, o, lse):
    vm, hbm = pl.BlockSpec(memory_space=pltpu.VMEM), pl.BlockSpec(memory_space=pltpu.HBM)
    bf, f32 = jnp.bfloat16, jnp.float32
    dma = pltpu.SemaphoreType.DMA
    shapes = (
        jax.ShapeDtypeStruct((HALF, 4 * HEADS, 128), bf),
        jax.ShapeDtypeStruct((BLK, OWN_HEADS, 128), bf),
        jax.ShapeDtypeStruct((BLK, OWN_HEADS, 128), bf),
    )
    grads = pl.pallas_call(
        lambda *refs: kernel(n_seq, *refs),
        out_shape=shapes,
        in_specs=[hbm] * 6,
        out_specs=(vm, vm, vm),
        scratch_shapes=[
            pltpu.VMEM((3, HALF, 4 * HEADS, 128), bf),
            pltpu.VMEM((BLK, OWN_HEADS, 128), bf),
            pltpu.VMEM((BLK, OWN_HEADS, 128), bf),
            pltpu.VMEM((4 * HEADS, HALF), f32),
            dma((6,)),
            pltpu.VMEM((OWN_HEADS, 2, BLK, 128), bf),
            pltpu.VMEM((OWN_HEADS, 2, BLK, 128), bf),
            pltpu.VMEM((HEADS, GROUP, 128), bf),
            pltpu.VMEM((HEADS, GROUP, 128), bf),
            pltpu.VMEM((HEADS, GROUP, 128), bf),
            pltpu.VMEM((HEADS, 1, GROUP), f32),
            pltpu.VMEM((HEADS, 1, GROUP), f32),
            pltpu.VMEM((HEADS, GROUP, 128), bf),
            pltpu.VMEM((HEADS, 2, 3 * BLK, 128), bf),
            pltpu.VMEM((HEADS, 2, 3 * BLK, 128), f32),
            pltpu.VMEM((HEADS, 2, BLK, 128), bf),
            pltpu.VMEM((HEADS, 2, BLK, 128), bf),
            pltpu.VMEM((OWN_HEADS, 2, BLK, 128), bf),
            pltpu.VMEM((HEADS, 2, BLK, 128), bf),
            pltpu.VMEM((HEADS, 2, BLK, 128), bf),
            pltpu.VMEM((OWN_HEADS, 2, BLK, 128), bf),
            dma((4,)), dma((4,)), dma((8,)), dma((8,)), dma((8,)), dma((8,)),
            dma((4,)), dma((4,)), dma((8,)), dma((8,)), dma((8,)), dma((8,)),
        ],
        compiler_params=pltpu.CompilerParams(
            collective_id=0, has_side_effects=True, vmem_limit_bytes=50 * 2**20
        ),
        name="window_grads",
    )(*(pltpu.with_memory_space_constraint(a, pltpu.HBM) for a in (k, v, q, do, o, lse)))
    return pl.pallas_call(
        store,
        out_shape=shapes,
        in_specs=[vm] * 3,
        out_specs=(hbm, hbm, hbm),
        scratch_shapes=[dma((3,))],
        compiler_params=pltpu.CompilerParams(vmem_limit_bytes=8 * 2**20),
        name="store_grads",
    )(*grads)


def body(n_seq, queries, keys, values, outputs, output_gradient, lse):
    return attention_grads(n_seq, keys, values, queries, output_gradient, outputs, lse.transpose(1, 0))


def solution(mesh):
    n_seq = mesh.shape["seq"]
    return jax.shard_map(
        lambda *args: body(n_seq, *args),
        mesh=mesh,
        in_specs=(
            P(("seq", "head"), None, None),
            P("seq", "head", None),
            P("seq", "head", None),
            P(("seq", "head"), None, None),
            P(("seq", "head"), None, None),
            P(("seq", "head"), None),
        ),
        out_specs=(P(("seq", "head"), None, None), P("seq", "head", None), P("seq", "head", None)),
        check_vma=False,
    )
```
